8 devices in a mesh: data: 2 (over z, y), stage: 4 (over x, core).
Axes of the slice: x: 2, y: 2, z: 1, core: 2. Of those that a mesh axis runs over, the one named last changes fastest.
Arguments:
- x: bfloat16 [32, 512, 1024], P('data'), parts along dimension 0
- g: bfloat16 [32, 512, 1024], P('data'), parts along dimension 0
- w1: bfloat16 [2, 4, 1024, 4096], P(None, 'stage')
- w2: bfloat16 [2, 4, 4096, 1024], P(None, 'stage')
Outputs:
- output 1: bfloat16 [32, 512, 1024], P('data'), parts along dimension 0
- output 2: bfloat16 [32, 512, 1024], P('data'), parts along dimension 0
- output 3: float32 [4, 4, 1024, 4096], P('data', 'stage'), parts along dimension 0
- output 4: float32 [4, 4, 4096, 1024], P('data', 'stage'), parts along dimension 0
There are 2 independent parts. The reference program is written for one: setup_inputs(seed, part) draws one part's arguments, and reference() takes and returns one part's arrays. A program takes and returns all parts, laid end to end along the dimension named above; an argument that names none is the same for every part.
All inputs are finite; a program needn't handle non-finite values.
Results may differ from the reference program's by a relative error of at most 0.02.
Values are sent between devices in bfloat16 or wider.
A program may use at most 1 GiB of HBM per device.

```python
import jax
import jax.numpy as jnp
from jax import lax

M = 16
B = 512
D = 1024
F = 4096
V = 2
S = 4


def gelu(z):
    return 0.5 * z * (1.0 + lax.erf(z * 0.7071067811865476))


def gelu_grad(z):
    return 0.5 * (1.0 + lax.erf(z * 0.7071067811865476)) + z * jnp.exp(-0.5 * z * z) * 0.3989422804014327


def setup_inputs(seed: int = 0, part: int = 0) -> dict:
    ks, kp = jax.random.split(jax.random.PRNGKey(seed))
    kx, kg = jax.random.split(jax.random.fold_in(kp, part))
    k1, k2 = jax.random.split(ks)
    nl = V * S
    x = jax.random.normal(kx, (M, B, D), jnp.float32).astype(jnp.bfloat16)
    g = jax.random.normal(kg, (M, B, D), jnp.float32).astype(jnp.bfloat16)
    w1 = (jax.random.normal(k1, (V, S, D, F), jnp.float32) * D ** -0.5).astype(jnp.bfloat16)
    w2 = (jax.random.normal(k2, (V, S, F, D), jnp.float32) * (2.0 / (nl * F) ** 0.5)).astype(jnp.bfloat16)
    return {'x': x, 'g': g, 'w1': w1, 'w2': w2}


def _layer_fwd(h, w1, w2):
    z = jnp.dot(h, w1, preferred_element_type=jnp.float32)
    u = gelu(z).astype(jnp.bfloat16)
    r = jnp.dot(u, w2, preferred_element_type=jnp.float32)
    return (h.astype(jnp.float32) + r).astype(jnp.bfloat16)


def _layer_bwd(h, w1, w2, dy):
    z = jnp.dot(h, w1, preferred_element_type=jnp.float32)
    u = gelu(z).astype(jnp.bfloat16)
    dw2 = jnp.dot(u.T, dy, preferred_element_type=jnp.float32)
    du = jnp.dot(dy, w2.T, preferred_element_type=jnp.float32)
    dz = (du * gelu_grad(z)).astype(jnp.bfloat16)
    dw1 = jnp.dot(h.T, dz, preferred_element_type=jnp.float32)
    dh = (dy.astype(jnp.float32) + jnp.dot(dz, w1.T, preferred_element_type=jnp.float32)).astype(jnp.bfloat16)
    return dh, dw1, dw2


def reference(x, g, w1, w2):
    w1s = w1.reshape(V * S, D, F)
    w2s = w2.reshape(V * S, F, D)

    def one(carry, xg):
        a1, a2 = carry
        xm, gm = xg

        def fwd(h, w):
            return _layer_fwd(h, w[0], w[1]), h

        y, hs = lax.scan(fwd, xm, (w1s, w2s))

        def bwd(dy, t):
            dh, d1, d2 = _layer_bwd(t[0], t[1], t[2], dy)
            return dh, (d1, d2)

        dx, (d1s, d2s) = lax.scan(bwd, gm, (hs, w1s, w2s), reverse=True)
        return (a1 + d1s, a2 + d2s), (y, dx)

    init = (jnp.zeros((V * S, D, F), jnp.float32), jnp.zeros((V * S, F, D), jnp.float32))
    (a1, a2), (y, dx) = lax.scan(one, init, (x, g))
    return y, dx, a1.reshape(V, S, D, F), a2.reshape(V, S, F, D)
```

```python
import functools

import jax
import jax.numpy as jnp
from jax import lax
from jax.experimental import pallas as pl
from jax.experimental.pallas import tpu as pltpu
from jax.sharding import PartitionSpec as P

MESH = pl.DeviceIdType.MESH
ANY = pl.ANY
BF = jnp.bfloat16
F32 = jnp.float32
VMEM_LIMIT = 67043328
NT = (((1,), (1,)), ((), ()))
TN = (((0,), (0,)), ((), ()))
HOUT = 4
DHO = 2


def _gelu(z):
    return 0.5 * z * (1.0 + lax.erf(z * 0.7071067811865476))


def _gelu_pair(z):
    half = 0.5 * (1.0 + lax.erf(z * 0.7071067811865476))
    return z * half, half + z * jnp.exp(-0.5 * z * z) * 0.3989422804014327


def _pipe_kernel(S, V, M, B, D, F, G, W0, WSTEP, YD, DXD, NS, FB,
                 x, g, w1, w2,
                 hs, dys, us, dzs, yo, dxo,
                 w1v, w2v, hin, hout, uf, hb, dyb, zb, ubuf, dzbuf, dho,
                 wsem, finsem, frecv, fsend, ysem, yrecv, yfwd,
                 hbsem, dysem, uosem, brecv, bsend, dxsem, dxrecv, dxfwd):
    p = lax.axis_index('stage')
    right = lax.rem(p + 1, S)
    left = lax.rem(p + S - 1, S)
    N = V * M
    HB = B // 2
    wp = W0 + WSTEP * (S - 1 - p)
    is_last = lax.div(p + 1, S)
    is_first = 1 - lax.div(p + S - 1, S)

    def unit_f(i):
        gi = lax.div(i, V * G)
        rem = lax.rem(i, V * G)
        return lax.div(rem, G), gi * G + lax.rem(rem, G)

    def unit_b(i):
        v, m = unit_f(i)
        return V - 1 - v, m

    def rdma(src, dst, ssem, rsem, to):
        return pltpu.make_async_remote_copy(src_ref=src, dst_ref=dst, send_sem=ssem, recv_sem=rsem,
                                            device_id={'stage': to}, device_id_type=MESH)

    def rows(q):
        return pl.ds(pl.multiple_of(q * HB, HB), HB)

    def f_send(s, v, m, q):
        sl = lax.rem(s, HOUT)
        return rdma(hout.at[sl, rows(q)], hs.at[v + is_last, m, rows(q)],
                    fsend.at[sl, q], frecv.at[v + is_last, m, q], right)

    def f_recv(v, m, q):
        return rdma(hout.at[0, rows(q)], hs.at[v, m, rows(q)], fsend.at[0, q], frecv.at[v, m, q], right)

    def f_load_x(s, m, q):
        sl = lax.rem(s, 2)
        return pltpu.make_async_copy(x.at[m, rows(q)], hin.at[sl, rows(q)], finsem.at[sl, q])

    def f_load_h(s, v, m, q):
        sl = lax.rem(s, 2)
        return pltpu.make_async_copy(hs.at[v, m, rows(q)], hin.at[sl, rows(q)], finsem.at[sl, q])

    def y_copies(s, m):
        sl = lax.rem(s, HOUT)
        return (pltpu.make_async_copy(hout.at[sl], yo.at[m], ysem.at[sl, 0]),
                rdma(hout.at[sl], yo.at[m], ysem.at[sl, 1], yrecv.at[m], left),
                rdma(hout.at[sl], yo.at[m], ysem.at[sl, 2], yrecv.at[m], right))

    def f_out_wait(s):
        v, m = unit_f(s)
        final = (is_last == 1) & (v == V - 1)

        @pl.when(final)
        def _():
            a, b, c = y_copies(s, m)
            a.wait()
            b.wait_send()
            c.wait_send()

        @pl.when(jnp.logical_not(final))
        def _():
            f_send(s, v, m, 0).wait_send()
            f_send(s, v, m, 1).wait_send()

    def b_send(b, v, m):
        sl = lax.rem(b, DHO)
        return rdma(dho.at[sl], dys.at[v - is_first, m], bsend.at[sl], brecv.at[v - is_first, m], left)

    def b_recv(v, m):
        return rdma(dho.at[0], dys.at[v, m], bsend.at[0], brecv.at[v, m], left)

    def dx_copies(b, m):
        sl = lax.rem(b, DHO)
        return (pltpu.make_async_copy(dho.at[sl], dxo.at[m], dxsem.at[sl, 0]),
                rdma(dho.at[sl], dxo.at[m], dxsem.at[sl, 1], dxrecv.at[m], left),
                rdma(dho.at[sl], dxo.at[m], dxsem.at[sl, 2], dxrecv.at[m], right))

    def b_out_wait(b):
        v, m = unit_b(b)
        final = (is_first == 1) & (v == 0)

        @pl.when(final)
        def _():
            a, c, d = dx_copies(b, m)
            a.wait()
            c.wait_send()
            d.wait_send()

        @pl.when(jnp.logical_not(final))
        def _():
            b_send(b, v, m).wait_send()

    def hb_start(b):
        v, m = unit_b(b)
        sl = lax.rem(b, 2)
        own = (is_first == 1) & (v == 0)

        @pl.when(own)
        def _():
            pltpu.make_async_copy(x.at[m], hb.at[sl], hbsem.at[sl]).start()

        @pl.when(jnp.logical_not(own))
        def _():
            pltpu.make_async_copy(hs.at[v, m], hb.at[sl], hbsem.at[sl]).start()

    def u_out(v, m):
        return (pltpu.make_async_copy(ubuf, us.at[v, m], uosem.at[0]),
                pltpu.make_async_copy(dzbuf, dzs.at[v, m], uosem.at[1]))

    def w_copies(v):
        return (pltpu.make_async_copy(w1.at[v], w1v.at[v], wsem.at[v, 0]),
                pltpu.make_async_copy(w2.at[v], w2v.at[v], wsem.at[v, 1]))

    @pl.when(is_first == 1)
    def _():
        f_load_x(0, 0, 0).start()
        f_load_x(0, 0, 1).start()

    for v in range(V):
        for c in w_copies(v):
            c.start()

    barrier = pltpu.get_barrier_semaphore()
    for nb in (left, right):
        pl.semaphore_signal(barrier, inc=1, device_id={'stage': nb}, device_id_type=MESH)
    pl.semaphore_wait(barrier, 2)

    for c in w_copies(0):
        c.wait()

    def slot(s, carry):
        @pl.when(s == G)
        def _():
            for v in range(1, V):
                for c in w_copies(v):
                    c.wait()

        def y_forward(i):
            v, m = unit_f(i)
            return (i >= 0) & (i < N) & (v == V - 1) & (is_first == 1), m

        def dx_forward(i):
            v, m = unit_b(i)
            return (i >= 0) & (i < N) & (v == 0) & (is_last == 1), m

        def y_fwd(m):
            return rdma(yo.at[m], yo.at[m], yfwd, yrecv.at[m], right)

        def dx_fwd(m):
            return rdma(dxo.at[m], dxo.at[m], dxfwd, dxrecv.at[m], left)

        was, mo = y_forward(s - 1 - YD)

        @pl.when(was)
        def _():
            y_fwd(mo).wait_send()

        was, mo = dx_forward(s - 1 - DXD)

        @pl.when(was)
        def _():
            dx_fwd(mo).wait_send()

        now, mn = y_forward(s - YD)

        @pl.when(now)
        def _():
            y_fwd(mn).wait_recv()
            y_fwd(mn).start()

        now, mn = dx_forward(s - DXD)

        @pl.when(now)
        def _():
            dx_fwd(mn).wait_recv()
            dx_fwd(mn).start()

        b = s - wp
        has_b = (b >= 0) & (b < N)
        has_f = s < N
        fv, fm = unit_f(s)
        f_own = (is_first == 1) & (fv == 0)

        @pl.when(has_f & has_b & f_own)
        def _():
            f_load_x(s, fm, 0).start()
            f_load_x(s, fm, 1).start()

        @pl.when(has_f & has_b & jnp.logical_not(f_own))
        def _():
            for q in range(2):
                f_recv(fv, fm, q).wait_recv()
                f_load_h(s, fv, fm, q).start()

        @pl.when(has_b)
        def _():
            v, m = unit_b(b)
            sl = lax.rem(b, 2)
            so = lax.rem(b, DHO)
            top = (is_last == 1) & (v == V - 1)

            @pl.when(top)
            def _():
                pltpu.make_async_copy(g.at[m], dyb, dysem).start()

            @pl.when(jnp.logical_not(top))
            def _():
                b_recv(v, m).wait_recv()
                pltpu.make_async_copy(dys.at[v, m], dyb, dysem).start()

            @pl.when(b == 0)
            def _():
                hb_start(b)

            @pl.when((s >= N) & (b + 1 < N))
            def _():
                hb_start(b + 1)

            @pl.when(b >= 1)
            def _():
                vo, mo = unit_b(b - 1)
                for c in u_out(vo, mo):
                    c.wait()

            @pl.when(b >= DHO)
            def _():
                b_out_wait(b - DHO)

            pltpu.make_async_copy(hs.at[v, m], hb.at[sl], hbsem.at[sl]).wait()
            h = hb[sl]
            zb[...] = jnp.dot(h, w1v[v, :, 0:FB], preferred_element_type=F32)
            pltpu.make_async_copy(g.at[m], dyb, dysem).wait()
            dy = dyb[...]
            for c in range(F // FB):
                cols = slice(c * FB, (c + 1) * FB)
                if c == 0:
                    z = zb[...]
                else:
                    z = jnp.dot(h, w1v[v, :, cols], preferred_element_type=F32)
                u, d = _gelu_pair(z)
                ubuf[:, cols] = u.astype(BF)
                du = lax.dot_general(dy, w2v[v, cols, :], NT, preferred_element_type=F32)
                dzbuf[:, cols] = (du * d).astype(BF)
            for c in u_out(v, m):
                c.start()
            r = lax.dot_general(dzbuf[...], w1v[v], NT, preferred_element_type=F32)
            dho[so] = (dy.astype(F32) + r).astype(BF)

            final = (is_first == 1) & (v == 0)

            @pl.when(final)
            def _():
                for c in dx_copies(b, m):
                    c.start()

            @pl.when(jnp.logical_not(final))
            def _():
                b_send(b, v, m).start()

        @pl.when(has_f)
        def _():
            sl = lax.rem(s, 2)
            so = lax.rem(s, HOUT)
            y_unit = (is_last == 1) & (fv == V - 1)

            @pl.when(s >= HOUT)
            def _():
                f_out_wait(s - HOUT)

            nv, nm = unit_f(s + 1)

            @pl.when((s + 1 < wp) & (is_first == 1) & (nv == 0))
            def _():
                f_load_x(s + 1, nm, 0).start()
                f_load_x(s + 1, nm, 1).start()

            def half(q, c2):
                @pl.when(jnp.logical_not(has_b) & jnp.logical_not(f_own))
                def _():
                    f_recv(fv, fm, q).wait_recv()
                    f_load_h(s, fv, fm, q).start()

                f_load_x(s, fm, q).wait()

                @pl.when((q == 1) & (s + 1 - wp >= 1) & (s + 1 - wp < N))
                def _():
                    hb_start(s + 1 - wp)

                h = hin[sl, rows(q), :]
                for c in range(F // FB):
                    cols = slice(c * FB, (c + 1) * FB)
                    z = jnp.dot(h, w1v[fv, :, cols], preferred_element_type=F32)
                    uf[:, cols] = _gelu(z).astype(BF)
                r = jnp.dot(uf[...], w2v[fv], preferred_element_type=F32)
                hout[so, rows(q), :] = (h.astype(F32) + r).astype(BF)

                @pl.when(jnp.logical_not(y_unit))
                def _():
                    f_send(s, fv, fm, q).start()

                return c2

            lax.fori_loop(0, 2, half, 0)

            @pl.when(y_unit)
            def _():
                for c in y_copies(s, fm):
                    c.start()

        return carry

    lax.fori_loop(0, NS, slot, 0)

    for i in range(N - HOUT, N):
        f_out_wait(i)
    for i in range(N - DHO, N):
        b_out_wait(i)
    vo, mo = unit_b(N - 1)
    for c in u_out(vo, mo):
        c.wait()

    mid = (is_first == 0) & (is_last == 0)

    def drain(m, carry):
        @pl.when(mid)
        def _():
            rdma(yo.at[m], yo.at[m], yfwd, yrecv.at[m], right).wait_recv()
            rdma(dxo.at[m], dxo.at[m], dxfwd, dxrecv.at[m], left).wait_recv()

        return carry

    lax.fori_loop(0, M, drain, 0)


def _pipe(x, g, w1, w2, S):
    M, B, D = x.shape
    V, _, F = w1.shape
    N = V * M
    G = M // 2
    W0, WSTEP = G + 1, 3
    YD, DXD = 8, 16
    NS = max(N + W0 + WSTEP * (S - 1), N + DXD + 1, N + YD + 1)
    FB = F // 4
    kern = functools.partial(_pipe_kernel, S, V, M, B, D, F, G, W0, WSTEP, YD, DXD, NS, FB)
    act = jax.ShapeDtypeStruct((V, M, B, D), BF)
    wide = jax.ShapeDtypeStruct((V, M, B, F), BF)
    out = jax.ShapeDtypeStruct((M, B, D), BF)
    DMA = pltpu.SemaphoreType.DMA
    flops = N * 10 * B * D * F
    return pl.pallas_call(
        kern,
        out_shape=(act, act, wide, wide, out, out),
        in_specs=[pl.BlockSpec(memory_space=ANY)] * 4,
        out_specs=[pl.BlockSpec(memory_space=ANY)] * 6,
        scratch_shapes=[
            pltpu.VMEM((V, D, F), BF), pltpu.VMEM((V, F, D), BF),
            pltpu.VMEM((2, B, D), BF), pltpu.VMEM((HOUT, B, D), BF), pltpu.VMEM((B // 2, F), BF),
            pltpu.VMEM((2, B, D), BF), pltpu.VMEM((B, D), BF), pltpu.VMEM((B, FB), F32),
            pltpu.VMEM((B, F), BF), pltpu.VMEM((B, F), BF), pltpu.VMEM((DHO, B, D), BF),
            DMA((V, 2)), DMA((2, 2)), DMA((V, M, 2)), DMA((HOUT, 2)), DMA((HOUT, 3)), DMA((M,)), DMA,
            DMA((2,)), DMA, DMA((2,)), DMA((V, M)), DMA((DHO,)), DMA((DHO, 3)), DMA((M,)), DMA,
        ],
        compiler_params=pltpu.CompilerParams(collective_id=0, has_side_effects=True, vmem_limit_bytes=VMEM_LIMIT),
        cost_estimate=pl.CostEstimate(flops=flops, bytes_accessed=N * B * (F * 4 + D * 12), transcendentals=0),
        name='pipe',
    )(x, g, w1, w2)


def _grad_kernel(S, V, M, B, D, F, FB, KM,
                 x, g, hs, dys, us, dzs, yo, dxo,
                 d1, d2, y, dx,
                 abuf, bbuf, acc, stage, asem, bsem, osem, ssem):
    p = lax.axis_index('stage')
    own_h = p == 0
    own_g = p == S - 1
    NF = F // FB
    NB = V * 2 * NF
    NK = M // KM

    def block(i):
        v = lax.div(i, 2 * NF)
        rem = lax.rem(i, 2 * NF)
        return v, lax.div(rem, NF), lax.rem(rem, NF)

    def fcols(f):
        return pl.ds(pl.multiple_of(f * FB, FB), FB)

    def load(i, k, start):
        v, w, f = block(i)
        sl = k % 2
        ms = pl.ds(k * KM, KM)

        def go(src, dst, sem):
            c = pltpu.make_async_copy(src, dst, sem)
            c.start() if start else c.wait()

        if not start:
            go(hs.at[0, ms], abuf.at[sl], asem.at[sl])
            go(hs.at[0, ms], bbuf.at[sl], bsem.at[sl])
            return

        @pl.when((w == 0) & own_h & (v == 0))
        def _():
            go(x.at[ms], abuf.at[sl], asem.at[sl])

        @pl.when((w == 0) & jnp.logical_not(own_h & (v == 0)))
        def _():
            go(hs.at[v, ms], abuf.at[sl], asem.at[sl])

        @pl.when(w == 0)
        def _():
            go(dzs.at[v, ms, :, fcols(f)], bbuf.at[sl], bsem.at[sl])

        @pl.when(w == 1)
        def _():
            go(us.at[v, ms, :, fcols(f)], abuf.at[sl], asem.at[sl])

        @pl.when((w == 1) & own_g & (v == V - 1))
        def _():
            go(g.at[ms], bbuf.at[sl], bsem.at[sl])

        @pl.when((w == 1) & jnp.logical_not(own_g & (v == V - 1)))
        def _():
            go(dys.at[v, ms], bbuf.at[sl], bsem.at[sl])

    def store(i, start):
        v, w, f = block(i)
        sl = lax.rem(i, 2)

        def go(dst):
            c = pltpu.make_async_copy(acc.at[sl], dst, osem.at[sl])
            c.start() if start else c.wait()

        if not start:
            go(d1.at[0, :, pl.ds(0, FB)])
            return

        @pl.when(w == 0)
        def _():
            go(d1.at[v, :, fcols(f)])

        @pl.when(w == 1)
        def _():
            go(d2.at[v, fcols(f), :])

    def pass_copies(m, out):
        if out:
            return (pltpu.make_async_copy(stage.at[0], y.at[m], ssem.at[0]),
                    pltpu.make_async_copy(stage.at[1], dx.at[m], ssem.at[1]))
        return (pltpu.make_async_copy(yo.at[m], stage.at[0], ssem.at[0]),
                pltpu.make_async_copy(dxo.at[m], stage.at[1], ssem.at[1]))

    load(0, 0, True)

    def step(i, carry):
        sl = lax.rem(i, 2)
        has_pass = i < M

        @pl.when(has_pass)
        def _():
            for c in pass_copies(lax.rem(i, M), False):
                c.start()

        @pl.when(i >= 2)
        def _():
            store(i - 2, False)

        for k in range(NK):
            if k + 1 < NK:
                load(i, k + 1, True)
            else:
                @pl.when(i + 1 < NB)
                def _():
                    load(i + 1, 0, True)
            load(i, k, False)
            part = lax.dot_general(abuf[k % 2].reshape(KM * B, D), bbuf[k % 2].reshape(KM * B, FB), TN,
                                   preferred_element_type=F32)
            if k == 0:
                acc[sl] = part
            else:
                acc[sl] += part
            if k == 0:
                @pl.when(has_pass)
                def _():
                    for c in pass_copies(lax.rem(i, M), False):
                        c.wait()
                    for c in pass_copies(lax.rem(i, M), True):
                        c.start()

        @pl.when(has_pass)
        def _():
            for c in pass_copies(lax.rem(i, M), True):
                c.wait()

        store(i, True)
        return carry

    lax.fori_loop(0, NB, step, 0)
    store(NB - 2, False)
    store(NB - 1, False)


def _grads(x, g, hs, dys, us, dzs, yo, dxo, S):
    V, M, B, F = us.shape
    D = x.shape[2]
    FB = D
    KM = M // 2
    NB = V * 2 * (F // FB)
    assert NB >= M and (M // KM) % 2 == 0
    kern = functools.partial(_grad_kernel, S, V, M, B, D, F, FB, KM)
    DMA = pltpu.SemaphoreType.DMA
    return pl.pallas_call(
        kern,
        out_shape=(jax.ShapeDtypeStruct((V, D, F), F32), jax.ShapeDtypeStruct((V, F, D), F32),
                   jax.ShapeDtypeStruct((M, B, D), BF), jax.ShapeDtypeStruct((M, B, D), BF)),
        in_specs=[pl.BlockSpec(memory_space=ANY)] * 8,
        out_specs=[pl.BlockSpec(memory_space=ANY)] * 4,
        scratch_shapes=[
            pltpu.VMEM((2, KM, B, D), BF), pltpu.VMEM((2, KM, B, FB), BF), pltpu.VMEM((2, D, FB), F32),
            pltpu.VMEM((2, B, D), BF), DMA((2,)), DMA((2,)), DMA((2,)), DMA((2,)),
        ],
        compiler_params=pltpu.CompilerParams(vmem_limit_bytes=VMEM_LIMIT),
        cost_estimate=pl.CostEstimate(flops=V * M * 4 * B * D * F, bytes_accessed=V * M * B * (4 * F + 4 * D),
                                      transcendentals=0),
        name='grads',
    )(x, g, hs, dys, us, dzs, yo, dxo)


def solution(mesh):
    S = mesh.shape['stage']

    def body(x, g, w1, w2):
        w1 = w1[:, 0]
        w2 = w2[:, 0]
        hs, dys, us, dzs, yo, dxo = _pipe(x, g, w1, w2, S)
        d1, d2, y, dx = _grads(x, g, hs, dys, us, dzs, yo, dxo, S)
        return y, dx, d1[:, None], d2[:, None]

    act = P('data', None, None)
    wsp = P(None, 'stage', None, None)
    gsp = P('data', 'stage', None, None)
    return jax.shard_map(body, mesh=mesh, in_specs=(act, act, wsp, wsp), out_specs=(act, act, gsp, gsp), check_vma=False)
```
